32 devices in a mesh: rate: 4 (over y, core), seq: 8 (over z, x).
Axes of the slice: x: 2, y: 2, z: 4, core: 2. Of those that a mesh axis runs over, the one named last changes fastest.
Arguments:
- queries: bfloat16 [8192, 16, 128], P('seq'), may hold values from -6 to 6
- key_rows: bfloat16 [8192, 16, 128], P('seq'), may hold values from -6 to 6
- values: bfloat16 [8192, 16, 128], P('seq'), may hold values from -6 to 6
- attn_out: bfloat16 [8192, 16, 128], P('seq'), may hold values from -6 to 6
- out_grad: bfloat16 [8192, 16, 128], P('seq'), may hold values from -6 to 6
- log_totals: float32 [8192, 16], P('seq'), as said below
- assignment: int32 [16], replicated, may hold values from 0 to 15, as said below
Outputs:
- query_grad: bfloat16 [8192, 16, 128], P('seq', 'rate')
- key_grad: bfloat16 [8192, 16, 128], P('seq', 'rate')
- value_grad: bfloat16 [8192, 16, 128], P('seq', 'rate')
The draws below stay inside these ranges and needn't reach their ends.
Inputs may be any that keep to these rules, and one draw needn't show every extreme that they name: `assignment`: each of the 16 heads appears once. `log_totals`: at each head's selected positions the natural logarithm of the sum of exp(scores) over the keys b <= a of its segment, computed from queries and key_rows; 0 at other positions.
All inputs are finite; a program needn't handle non-finite values.
Results may differ from the reference program's by a relative error of at most 0.0049.
Values may be sent and summed in bfloat16 or wider, within the bound.
No kernel may reach another device: no remote copies, remote signals or barrier semaphores. Data moves between devices by JAX's collectives and lax.ppermute only.
A program may use at most 128 MiB of HBM per device.

```python
import jax
import jax.numpy as jnp
from jax import lax

HEADS = 16
HEAD_DIM = 128
SEG = 2048
TOKENS = 8192


def base_draw(seed_key):
    permuted = jax.random.permutation(jax.random.fold_in(seed_key, 101), HEADS).astype(jnp.int32)
    full_shape = (TOKENS, HEADS, HEAD_DIM)
    query_draw = jnp.clip(jax.random.normal(jax.random.fold_in(seed_key, 102), full_shape), -6.0, 6.0)
    key_draw = jnp.clip(jax.random.normal(jax.random.fold_in(seed_key, 103), full_shape), -6.0, 6.0)
    return (permuted, query_draw.astype(jnp.bfloat16), key_draw.astype(jnp.bfloat16))


def segment_totals(operands, scaling):
    query_seg, key_seg = operands
    scores = jnp.dot(query_seg, key_seg.T, preferred_element_type=jnp.float32) * scaling
    positions = jnp.arange(query_seg.shape[0], dtype=jnp.int32)
    causal = positions[:, None] >= positions[None, :]
    return jax.nn.logsumexp(jnp.where(causal, scores, -1e+30), axis=1)


def draw_assignment(key, part):
    return base_draw(key)[0]


def draw_queries(key, part):
    return base_draw(key)[1]


def draw_key_rows(key, part):
    return base_draw(key)[2]


def draw_log_totals(key, part):
    permuted, query_draw, key_draw = base_draw(key)
    scaling = HEAD_DIM ** (-0.5)
    group_size = HEADS // 4
    totals_list = []
    for slot_index in range(HEADS):
        dilation = 2 ** (slot_index // group_size)
        offset = slot_index % group_size % dilation
        head_index = permuted[slot_index]
        seg_rows = min(SEG, TOKENS // dilation)
        query_col = lax.dynamic_index_in_dim(query_draw, head_index, 1, keepdims=False)
        key_col = lax.dynamic_index_in_dim(key_draw, head_index, 1, keepdims=False)
        query_sel = query_col.reshape(TOKENS // dilation, dilation, HEAD_DIM)[:, offset].reshape(-1, seg_rows, HEAD_DIM)
        key_sel = key_col.reshape(TOKENS // dilation, dilation, HEAD_DIM)[:, offset].reshape(-1, seg_rows, HEAD_DIM)
        totals = lax.map(lambda operands: segment_totals(operands, scaling), (query_sel, key_sel)).reshape(-1)
        column = jnp.zeros((TOKENS // dilation, dilation), jnp.float32).at[:, offset].set(totals)
        totals_list.append(column.reshape(TOKENS))
    inverse = jnp.argsort(permuted).astype(jnp.int32)
    return jnp.stack(totals_list, axis=1)[:, inverse]


def block_levels(key, shape, split, least, top_value):
    level = 1.0
    for position, shards_of in split:
        steps = jax.random.uniform(jax.random.fold_in(jax.random.fold_in(key, 6), position), (shards_of,), jnp.float32, least / len(split), top_value / len(split))
        level = level * jnp.repeat(jnp.exp(steps), shape[position] // shards_of).reshape((-1,) + (1,) * (len(shape) - 1 - position))
    return level


def centred(own_key, shape, scale, bound, cuts=(), kind=jnp.bfloat16):
    values = jax.random.normal(own_key, shape, jnp.float32) * scale
    if len(cuts) > 0:
        values = block_levels(own_key, shape, cuts, -0.22, 0.18) * values
    return jnp.clip(values, min=-bound, max=bound).astype(kind)


def setup_inputs(seed: int = 0) -> dict:
    arg_keys = jax.random.split(jax.random.key(seed), 8)
    queries = draw_queries(jax.random.fold_in(arg_keys[7], 71), 0)
    key_rows = draw_key_rows(jax.random.fold_in(arg_keys[7], 71), 0)
    values = centred(arg_keys[2], (TOKENS, HEADS, HEAD_DIM), 1.0, 6.0, ((0, 8),))
    attn_out = centred(arg_keys[3], (TOKENS, HEADS, HEAD_DIM), 1.0, 6.0, ((0, 8),))
    out_grad = centred(arg_keys[4], (TOKENS, HEADS, HEAD_DIM), 1.0, 6.0, ((0, 8),))
    log_totals = draw_log_totals(jax.random.fold_in(arg_keys[7], 71), 0)
    assignment = draw_assignment(jax.random.fold_in(arg_keys[7], 71), 0)
    return dict(queries=queries, key_rows=key_rows, values=values, attn_out=attn_out, out_grad=out_grad, log_totals=log_totals, assignment=assignment)


def segment_grads(operands, scaling):
    query_seg, key_seg, value_seg, grad_seg, total_seg, delta_seg = operands
    scores = jnp.dot(query_seg, key_seg.T, preferred_element_type=jnp.float32) * scaling
    count_rows = query_seg.shape[0]
    positions = jnp.arange(count_rows, dtype=jnp.int32)
    causal = positions[:, None] >= positions[None, :]
    probs = jnp.where(causal, jnp.exp(scores - total_seg[:, None]), 0.0)
    value_part = jnp.dot(probs.astype(jnp.bfloat16).T, grad_seg, preferred_element_type=jnp.float32)
    dprobs = jnp.dot(grad_seg, value_seg.T, preferred_element_type=jnp.float32)
    dscores = (probs * (dprobs - delta_seg[:, None])).astype(jnp.bfloat16)
    query_part = jnp.dot(dscores, key_seg, preferred_element_type=jnp.float32) * scaling
    key_part = jnp.dot(dscores.T, query_seg, preferred_element_type=jnp.float32) * scaling
    return query_part, key_part, value_part


def reference(queries, key_rows, values, attn_out, out_grad, log_totals, assignment):
    scaling = HEAD_DIM ** -0.5
    delta_rows = jnp.sum(out_grad.astype(jnp.float32) * attn_out.astype(jnp.float32), axis=2)
    group_size = HEADS // 4
    grad_columns = ([], [], [])
    for slot_index in range(HEADS):
        dilation = 2 ** (slot_index // group_size)
        offset = (slot_index % group_size) % dilation
        head_index = assignment[slot_index]
        picked = []
        for source_array in (queries, key_rows, values, out_grad):
            column = lax.dynamic_index_in_dim(source_array, head_index, 1, keepdims=False)
            picked.append(column.reshape(TOKENS // dilation, dilation, HEAD_DIM)[:, offset])
        for source_array in (log_totals, delta_rows):
            column = lax.dynamic_index_in_dim(source_array, head_index, 1, keepdims=False)
            picked.append(column.reshape(TOKENS // dilation, dilation)[:, offset])
        seg_rows = min(SEG, TOKENS // dilation)
        shaped = tuple(picked_item.reshape((-1, seg_rows) + picked_item.shape[1:]) for picked_item in picked)
        seg_parts = lax.map(lambda operands: segment_grads(operands, scaling), shaped)
        for which_grad in range(3):
            flat_rows = seg_parts[which_grad].reshape(TOKENS // dilation, HEAD_DIM)
            spread = jnp.zeros((TOKENS // dilation, dilation, HEAD_DIM), jnp.float32).at[:, offset].set(flat_rows)
            grad_columns[which_grad].append(spread.reshape(TOKENS, HEAD_DIM).astype(jnp.bfloat16))
    inverse = jnp.argsort(assignment).astype(jnp.int32)
    query_grad = jnp.stack(grad_columns[0], axis=1)[:, inverse]
    key_grad = jnp.stack(grad_columns[1], axis=1)[:, inverse]
    value_grad = jnp.stack(grad_columns[2], axis=1)[:, inverse]
    return (query_grad, key_grad, value_grad)
```

```python
import math

import jax
import jax.numpy as jnp
from jax import lax
from jax.experimental import pallas as pl
from jax.experimental.pallas import tpu as pltpu
from jax.sharding import PartitionSpec as P


HEADS = 16
SEG = 2048
LEVELS = 4
GROUPS = ((0,), (1,), (2, 3))
LANES = 128
TAG_ROWS = 16
LOG2E = math.log2(math.e)


F32 = jnp.float32
BF16 = jnp.bfloat16


def swapped(array, axis, by):
    devices = lax.axis_size(axis)
    return lax.ppermute(array, axis, [(i, i ^ by) for i in range(devices)])


def rows_dot(a, b):
    return lax.dot_general(a, b, (((1,), (1,)), ((), ())), preferred_element_type=F32)


def plain_dot(a, b):
    return jnp.dot(a, b, preferred_element_type=F32)


class Level:
    def __init__(self, level, local_tokens, all_tokens):
        self.rate = 2**level
        self.rows = local_tokens // self.rate
        self.span = min(SEG, all_tokens // self.rate) * self.rate // local_tokens
        self.bits = self.span.bit_length() - 1
        self.tags = self.rows // LANES * TAG_ROWS
        self.pack_rows = 2 * self.rows + self.tags


def pack_layout(levels, members, bit):
    at, offsets = 0, {}
    for level in members:
        if bit < levels[level].bits:
            offsets[level] = at
            at += levels[level].pack_rows
    return offsets, at


def split3(col):
    hi = col.astype(BF16).astype(F32)
    rest = col - hi
    mid = rest.astype(BF16).astype(F32)
    return hi, mid, rest - mid


def extract_kernel(levels, groups, group_size, sm, keys, values, queries, grads, outs, logs, *refs):
    members = [m for group in groups for m in group]
    n = len(members)
    own_refs, tag_refs, col_refs = refs[:n], refs[n : 2 * n], refs[2 * n : 3 * n]
    at = 3 * n
    send_refs = {}
    for group in groups:
        for bit in range(group_bits(levels, group)):
            send_refs[group, bit] = refs[at]
            at += 1
    bufs = refs[at : at + n]
    turned, sems = refs[at + n :]
    rho, seq = lax.axis_index("rate"), lax.axis_index("seq")
    tokens = keys.shape[0]
    sources = (keys, values, queries, grads, outs)
    copies = []
    for w, level in enumerate(members):
        rate, rows = levels[level].rate, levels[level].rows
        head = sm[level * group_size + rho]
        off = rho & (rate - 1)
        for s, source in enumerate(sources):
            picked = source.reshape(rows, rate, HEADS // 2, 2, LANES).at[:, off, head // 2]
            copy = pltpu.make_async_copy(picked, bufs[w].at[s], sems.at[w, s])
            copy.start()
            copies.append(copy)
    for u in range(tokens // LANES):
        part = logs[:, u * LANES : (u + 1) * LANES]
        square = jnp.concatenate([part, jnp.zeros((LANES - HEADS, LANES), F32)], axis=0)
        turned[u * LANES : (u + 1) * LANES, :] = square.T
    row_id = lax.broadcasted_iota(jnp.int32, (LANES, 2 * LANES), 0)
    col_id = lax.broadcasted_iota(jnp.int32, (LANES, 2 * LANES), 1)
    lane = lax.broadcasted_iota(jnp.int32, (LANES, LANES), 1)
    group_of = {m: group for group in groups for m in group}
    for w, level in enumerate(members):
        lv = levels[level]
        group = group_of[level]
        head = sm[level * group_size + rho]
        off = rho & (lv.rate - 1)
        pick = (col_id == 2 * row_id + head % 2).astype(BF16)
        for s in range(len(sources)):
            copies[w * len(sources) + s].wait()
        flat = [bufs[w].at[s].reshape(2 * lv.rows, LANES) for s in range(len(sources))]
        for u in range(lv.rows // LANES):
            got = [
                plain_dot(pick, flat[s][u * 2 * LANES : (u + 1) * 2 * LANES, :])
                for s in range(len(sources))
            ]
            delta = jnp.sum(got[3] * got[4], axis=1, keepdims=True)
            start = u * LANES * lv.rate + off
            if lv.rate == 1:
                logs_u = turned[u * LANES : (u + 1) * LANES, :]
            else:
                logs_u = turned[pl.ds(start, LANES, stride=lv.rate), :]
            total = jnp.sum(jnp.where(lane == head, logs_u, 0.0), axis=1, keepdims=True) * LOG2E
            square = jnp.zeros((LANES, LANES), F32)
            for at, col in enumerate(split3(total) + split3(delta) + (total, delta)):
                square = jnp.where(lane == at, col, square)
            col_refs[w][u * LANES : (u + 1) * LANES, :] = square
            tags = square.T[:TAG_ROWS].astype(BF16)
            tag_refs[w][u * TAG_ROWS : (u + 1) * TAG_ROWS, :] = tags
            low = [g.astype(BF16) for g in got[:4]]
            for s in range(4):
                own_refs[w][s * lv.rows + u * LANES : s * lv.rows + (u + 1) * LANES, :] = low[s]
            for bit in range(lv.bits):
                base = pack_layout(levels, group, bit)[0][level]
                later = (seq >> bit) % 2 == 1
                send = send_refs[group, bit]
                for s in range(2):
                    first = base + s * lv.rows + u * LANES
                    send[first : first + LANES, :] = jnp.where(later, low[2 + s], low[s])
                first = base + 2 * lv.rows + u * TAG_ROWS
                send[first : first + TAG_ROWS, :] = tags


def group_bits(levels, group):
    return max(levels[m].bits for m in group)


def extract(levels, groups, group_size, sm, sources, logs):
    tokens = sources[0].shape[0]
    members = [m for group in groups for m in group]
    n = len(members)
    shapes = [jax.ShapeDtypeStruct((4 * levels[m].rows, LANES), BF16) for m in members]
    shapes += [jax.ShapeDtypeStruct((levels[m].tags, LANES), BF16) for m in members]
    shapes += [jax.ShapeDtypeStruct((levels[m].rows, LANES), F32) for m in members]
    sent = [(group, bit) for group in groups for bit in range(group_bits(levels, group))]
    shapes += [
        jax.ShapeDtypeStruct((pack_layout(levels, group, bit)[1], LANES), BF16)
        for group, bit in sent
    ]

    def kernel(*refs):
        extract_kernel(levels, groups, group_size, *refs)

    results = pl.pallas_call(
        kernel,
        out_shape=shapes,
        in_specs=[pl.BlockSpec(memory_space=pltpu.SMEM)]
        + [pl.BlockSpec(memory_space=pl.ANY)] * 5
        + [pl.BlockSpec(memory_space=pltpu.VMEM)],
        scratch_shapes=[pltpu.VMEM((5, levels[m].rows, 2, LANES), BF16) for m in members]
        + [pltpu.VMEM((tokens, LANES), F32), pltpu.SemaphoreType.DMA((n, 5))],
    )(sm, *sources, logs)
    kept = {m: (results[w], results[n + w], results[2 * n + w]) for w, m in enumerate(members)}
    return kept, dict(zip(sent, results[3 * n :]))


def tag_row(tags, first_row, count, which):
    parts = []
    for u in range(count // LANES):
        at = pl.multiple_of(first_row // LANES * TAG_ROWS + u * TAG_ROWS, TAG_ROWS)
        tile = tags[pl.ds(at, TAG_ROWS), :].astype(F32)
        parts.append(tile[which : which + 1] + tile[which + 1 : which + 2] + tile[which + 2 : which + 3])
    return parts[0] if len(parts) == 1 else jnp.concatenate(parts, axis=1)


def query_side(q, g, total, delta, k, v, factor, allowed):
    scores = rows_dot(q, k)
    probs = jnp.exp2(scores * factor - total)
    if allowed is not None:
        probs = jnp.where(allowed, probs, 0.0)
    ds = (probs * (rows_dot(g, v) - delta)).astype(BF16)
    return plain_dot(ds, k)


def key_side(k, v, q, g, total, delta, factor, allowed):
    scores = rows_dot(k, q)
    probs = jnp.exp2(scores * factor - total)
    if allowed is not None:
        probs = jnp.where(allowed, probs, 0.0)
    dv = plain_dot(probs.astype(BF16), g)
    ds = (probs * (rows_dot(v, g) - delta)).astype(BF16)
    return plain_dot(ds, q), dv


class Block:
    def __init__(self, ref, first, second, tag_ref, tag_base):
        self.ref, self.first, self.second = ref, first, second
        self.tag_ref, self.tag_base = tag_ref, tag_base

    def pair(self, at, tile):
        def load(base):
            return self.ref[pl.ds(pl.multiple_of(base + at, TAG_ROWS), tile), :]

        return load(self.first), load(self.second)

    def tags(self, at, tile):
        base = self.tag_base // TAG_ROWS * LANES
        return tag_row(self.tag_ref, base + at, tile, 0), tag_row(self.tag_ref, base + at, tile, 3)


def run_tiles(count, tile, step):
    if count == 1:
        step(0)
        return

    def turn(i, carry):
        step(pl.multiple_of(i * tile, tile))
        return carry

    lax.fori_loop(0, count, turn, 0)


class LevelWork:
    def __init__(self, lv, own, tags, col, acc, at, scaling):
        self.rows, self.acc, self.at, self.col = lv.rows, acc, at, col
        self.tile = min(lv.rows, 256)
        self.count = lv.rows // self.tile
        self.factor = scaling * LOG2E
        self.keys = Block(own, 0, lv.rows, None, 0)
        self.queries = Block(own, 2 * lv.rows, 3 * lv.rows, tags, 0)

    def put(self, which, at, value, add):
        first = self.at + which * self.rows + at
        where = pl.ds(pl.multiple_of(first, TAG_ROWS), self.tile)
        if add:
            self.acc[where, :] += value
        else:
            self.acc[where, :] = value

    def query_rows(self, at):
        q, g = self.queries.pair(at, self.tile)
        where = pl.ds(at, self.tile)
        return q, g, self.col[where, 6:7], self.col[where, 7:8]

    def diagonal(self):
        tile = self.tile
        tri_r = lax.broadcasted_iota(jnp.int32, (tile, tile), 0)
        tri_c = lax.broadcasted_iota(jnp.int32, (tile, tile), 1)
        for i in range(self.count):
            mine = self.query_rows(i * tile)
            sum_q = jnp.zeros((tile, LANES), F32)
            for j in range(i + 1):
                allowed = tri_c <= tri_r if i == j else None
                sum_q += query_side(*mine, *self.keys.pair(j * tile, tile), self.factor, allowed)
            self.put(0, i * tile, sum_q, False)
            mine = self.keys.pair(i * tile, tile)
            sum_k = jnp.zeros((tile, LANES), F32)
            sum_v = jnp.zeros((tile, LANES), F32)
            for j in range(i, self.count):
                allowed = tri_r <= tri_c if i == j else None
                there = self.queries.pair(j * tile, tile) + self.queries.tags(j * tile, tile)
                part = key_side(*mine, *there, self.factor, allowed)
                sum_k += part[0]
                sum_v += part[1]
            self.put(1, i * tile, sum_k, False)
            self.put(2, i * tile, sum_v, False)

    def earlier_keys(self, blocks):
        def step(at):
            mine = self.query_rows(at)
            sum_q = jnp.zeros((self.tile, LANES), F32)
            for block in blocks:
                for j in range(self.count):
                    there = block.pair(j * self.tile, self.tile)
                    sum_q += query_side(*mine, *there, self.factor, None)
            self.put(0, at, sum_q, True)

        run_tiles(self.count, self.tile, step)

    def later_queries(self, blocks):
        def step(at):
            mine = self.keys.pair(at, self.tile)
            sum_k = jnp.zeros((self.tile, LANES), F32)
            sum_v = jnp.zeros((self.tile, LANES), F32)
            for block in blocks:
                for j in range(self.count):
                    there = block.pair(j * self.tile, self.tile) + block.tags(j * self.tile, self.tile)
                    part = key_side(*mine, *there, self.factor, None)
                    sum_k += part[0]
                    sum_v += part[1]
            self.put(1, at, sum_k, True)
            self.put(2, at, sum_v, True)

        run_tiles(self.count, self.tile, step)


def compute(levels, members, bits, kept, received, before, after, last, scaling):
    n = len(members)
    steps = [k for k in sorted(received) if k.bit_length() - 1 in bits]
    total_rows = 3 * sum(levels[m].rows for m in members)
    given = [kept[m][part] for part in range(3) for m in members]
    given += [received[k] for k in steps]
    if before is not None:
        given.append(before)
    inputs = len(given)

    def kernel(*refs):
        own_refs, tag_refs, col_refs = refs[:n], refs[n : 2 * n], refs[2 * n : 3 * n]
        got = dict(zip(steps, refs[3 * n :]))
        out = refs[inputs + len(after)]
        acc = refs[inputs + len(after) + 1] if last else out
        seq = lax.axis_index("seq")
        if before is not None:
            acc[...] = refs[inputs - 1][...]
        work, at = [], 0
        for w, level in enumerate(members):
            lv = levels[level]
            work.append(LevelWork(lv, own_refs[w], tag_refs[w], col_refs[w], acc, at, scaling))
            at += 3 * lv.rows
        if before is None:
            for each in work:
                each.diagonal()
        for bit in bits:
            later = (seq >> bit) % 2 == 1
            offsets = pack_layout(levels, members, bit)[0]
            todo = []
            for w, level in enumerate(members):
                if level in offsets:
                    rows, base = levels[level].rows, offsets[level]
                    todo.append(
                        (
                            work[w],
                            [
                                Block(got[k], base, base + rows, got[k], base + 2 * rows)
                                for k in range(2**bit, 2 ** (bit + 1))
                            ],
                        )
                    )

            @pl.when(later)
            def _(todo=todo):
                for each, blocks in todo:
                    each.earlier_keys(blocks)

            @pl.when(jnp.logical_not(later))
            def _(todo=todo):
                for each, blocks in todo:
                    each.later_queries(blocks)

        if last:
            at = 0
            for level in members:
                rows = levels[level].rows
                out[at : at + 2 * rows, :] = (acc[at : at + 2 * rows, :] * scaling).astype(BF16)
                out[at + 2 * rows : at + 3 * rows, :] = acc[at + 2 * rows : at + 3 * rows, :].astype(BF16)
                at += 3 * rows

    return pl.pallas_call(
        kernel,
        out_shape=jax.ShapeDtypeStruct((total_rows, LANES), BF16 if last else F32),
        in_specs=[pl.BlockSpec(memory_space=pltpu.VMEM)] * inputs
        + [pl.BlockSpec(memory_space=pl.ANY)] * len(after),
        scratch_shapes=[pltpu.VMEM((total_rows, LANES), F32)] if last else [],
    )(*given, *after)


def place(levels, group_size, heads_here, local_tokens, sm, gathered):
    rates = len(gathered[0])
    flat = [array for group in gathered for array in group]
    block, half = LANES, LANES // 2
    steps = local_tokens // block
    tall = heads_here * half

    def kernel(sm_ref, *refs):
        sources = refs[: len(flat)]
        outs = refs[len(flat) : len(flat) + 3]
        spread, buf, sems = refs[len(flat) + 3 :]
        step = pl.program_id(0)
        rho = lax.axis_index("rate")
        slots = []
        for i in range(heads_here):
            slot = jnp.int32(0)
            for s in range(HEADS):
                slot = jnp.where(sm_ref[s] == rho * heads_here + i, s, slot)
            slots.append(slot)
        shifts = [slot // group_size for slot in slots]

        @pl.when(step == 0)
        def _():
            for i in range(heads_here):
                for level in range(1, LEVELS):
                    end = 3 * levels[level].rows
                    buf[i, end : end + block, :] = jnp.zeros((block, LANES), BF16)

            def each(act):
                for i in range(heads_here):
                    lane_i = slots[i] % group_size
                    for g, members in enumerate(GROUPS):
                        at = 0
                        for level in members:
                            rows = 3 * levels[level].rows
                            for x in range(rates):
                                hit = jnp.logical_and(shifts[i] == level, lane_i == rho ^ x)

                                @pl.when(hit)
                                def _(i=i, g=g, x=x, at=at, rows=rows):
                                    act(
                                        pltpu.make_async_copy(
                                            sources[g * rates + x].at[pl.ds(at, rows)],
                                            buf.at[i, pl.ds(0, rows)],
                                            sems.at[i],
                                        )
                                    )

                            at += rows

            each(lambda copy: copy.start())
            row_id = lax.broadcasted_iota(jnp.int32, (tall, half), 0)
            col_id = lax.broadcasted_iota(jnp.int32, (tall, half), 1)
            for part in range(2):
                for i in range(heads_here):
                    rate = 1 << shifts[i]
                    off = (slots[i] % group_size) & (rate - 1)
                    first = jnp.where(shifts[i] == 0, 0, part * half)
                    token = col_id * rate + (off - first)
                    hit = row_id == token * heads_here + i
                    spread[part, :, i * half : (i + 1) * half] = hit.astype(BF16)
            each(lambda copy: copy.wait())

        for part in range(2):
            columns = []
            for which in range(3):
                rows = []
                for i in range(heads_here):
                    at = which * (local_tokens >> shifts[i]) + step * (block >> shifts[i])
                    at += jnp.where(shifts[i] == 0, part * half, 0)
                    rows.append(buf[i, pl.ds(pl.multiple_of(at, TAG_ROWS), half), :])
                columns.append(jnp.concatenate(rows, axis=0))
            two = plain_dot(spread[part], jnp.concatenate(columns[:2], axis=1))
            where = pl.ds(part * tall, tall)
            outs[0][where, :] = two[:, :LANES].astype(BF16)
            outs[1][where, :] = two[:, LANES:].astype(BF16)
            outs[2][where, :] = plain_dot(spread[part], columns[2]).astype(BF16)

    shape = jax.ShapeDtypeStruct((local_tokens * heads_here, LANES), BF16)
    spec = pl.BlockSpec((block * heads_here, LANES), lambda i: (i, 0))
    results = pl.pallas_call(
        kernel,
        grid=(steps,),
        out_shape=[shape] * 3,
        in_specs=[pl.BlockSpec(memory_space=pltpu.SMEM)]
        + [pl.BlockSpec(memory_space=pl.ANY)] * len(flat),
        out_specs=[spec] * 3,
        scratch_shapes=[
            pltpu.VMEM((2, tall, tall), BF16),
            pltpu.VMEM((heads_here, 3 * local_tokens + block, LANES), BF16),
            pltpu.SemaphoreType.DMA((heads_here,)),
        ],
        name="place",
    )(sm, *flat)
    return tuple(r.reshape(local_tokens, heads_here, LANES) for r in results)


def body(queries, key_rows, values, attn_out, out_grad, log_totals, assignment):
    local_tokens = queries.shape[0]
    scaling = queries.shape[2] ** (-0.5)
    rate_count = lax.axis_size("rate")
    seq_count = lax.axis_size("seq")
    group_size = HEADS // LEVELS
    levels = [Level(c, local_tokens, local_tokens * seq_count) for c in range(LEVELS)]
    paired = [
        a.reshape(local_tokens, HEADS // 2, 2, LANES)
        for a in (key_rows, values, queries, out_grad, attn_out)
    ]
    logs = log_totals.T
    kept, received = {}, {}
    for groups in (GROUPS[:1], GROUPS[1:]):
        some, sends = extract(levels, groups, group_size, assignment, paired, logs)
        kept.update(some)
        for members in groups:
            received[members] = {}
            for k in range(1, 2 ** group_bits(levels, members)):
                got = swapped(sends[members, k.bit_length() - 1], "seq", k)
                received[members][k] = got
    gathered = []
    for members in GROUPS:
        bits = list(range(group_bits(levels, members)))
        after = [kept[GROUPS[-1][-1]][1]] if members == GROUPS[0] else []
        split = 2 if len(bits) > 2 else len(bits)
        mine = None
        for part in (bits[:split], bits[split:]):
            if part:
                mine = compute(
                    levels,
                    members,
                    part,
                    kept,
                    received[members],
                    mine,
                    after,
                    part[-1] == bits[-1],
                    scaling,
                )
        far = swapped(mine, "rate", 2)
        gathered.append([mine, swapped(mine, "rate", 1), far, swapped(far, "rate", 1)])
    return place(levels, group_size, HEADS // rate_count, local_tokens, assignment, gathered)


def solution(mesh):
    placed = (P("seq", None, None),) * 5 + (P("seq", None), P())
    return jax.shard_map(
        body,
        mesh=mesh,
        in_specs=placed,
        out_specs=(P("seq", "rate", None),) * 3,
        check_vma=False,
    )
```

```python
import math

import jax
import jax.numpy as jnp
from jax import lax
from jax.experimental import pallas as pl
from jax.experimental.pallas import tpu as pltpu
from jax.sharding import PartitionSpec as P


HEADS = 16
SEG = 2048
LEVELS = 4
GROUPS = ((0,), (1,), (2, 3))
SENDS = ((0,), (1, 2, 3))
VMEM_LIMIT = 24 * 1024 * 1024
LANES = 128
TAG_ROWS = 8
PAIR = 16
LOG2E = math.log2(math.e)


F32 = jnp.float32
BF16 = jnp.bfloat16


def swapped(array, axis, by):
    devices = lax.axis_size(axis)
    return lax.ppermute(array, axis, [(i, i ^ by) for i in range(devices)])


def rows_dot(a, b):
    return lax.dot_general(a, b, (((1,), (1,)), ((), ())), preferred_element_type=F32)


def plain_dot(a, b):
    return jnp.dot(a, b, preferred_element_type=F32)


class Level:
    def __init__(self, level, local_tokens, all_tokens):
        self.rate = 2**level
        self.rows = local_tokens // self.rate
        self.span = min(SEG, all_tokens // self.rate) * self.rate // local_tokens
        self.bits = self.span.bit_length() - 1
        self.tags = max(self.rows // LANES * TAG_ROWS, PAIR)
        self.pack_rows = 2 * self.rows + self.tags


def pack_layout(levels, members, bit):
    at, offsets = 0, {}
    for level in members:
        if bit < levels[level].bits:
            offsets[level] = at
            at += levels[level].pack_rows
    return offsets, at


def split3(col):
    hi = col.astype(BF16).astype(F32)
    rest = col - hi
    mid = rest.astype(BF16).astype(F32)
    return hi, mid, rest - mid


def extract_kernel(levels, groups, group_size, sm, keys, values, queries, grads, outs, logs, *refs):
    members = [m for group in groups for m in group]
    n = len(members)
    own_refs, tag_refs, col_refs = refs[:n], refs[n : 2 * n], refs[2 * n : 3 * n]
    at = 3 * n
    send_refs = {}
    for group in groups:
        for bit in range(group_bits(levels, group)):
            send_refs[group, bit] = refs[at]
            at += 1
    bufs = refs[at : at + n]
    turned, logs_buf, logs_sem, sems = refs[at + n :]
    rho, seq = lax.axis_index("rate"), lax.axis_index("seq")
    tokens = keys.shape[0]
    sources = (keys, values, queries, grads, outs)
    copies = []
    for w, level in enumerate(members):
        rate, rows = levels[level].rate, levels[level].rows
        head = sm[level * group_size + rho]
        off = rho & (rate - 1)
        for s, source in enumerate(sources):
            picked = source.reshape(rows, rate, HEADS // 2, 2, LANES).at[:, off, head // 2]
            copy = pltpu.make_async_copy(picked, bufs[w].at[s], sems.at[w, s])
            copy.start()
            copies.append(copy)
        if w == 0:
            logs_copy = pltpu.make_async_copy(logs, logs_buf, logs_sem)
            logs_copy.start()
    logs_copy.wait()
    for u in range(tokens // LANES):
        part = logs_buf[:, u * LANES : (u + 1) * LANES]
        square = jnp.concatenate([part, jnp.zeros((LANES - HEADS, LANES), F32)], axis=0)
        turned[u * LANES : (u + 1) * LANES, :] = square.T
    row_id = lax.broadcasted_iota(jnp.int32, (LANES, 2 * LANES), 0)
    col_id = lax.broadcasted_iota(jnp.int32, (LANES, 2 * LANES), 1)
    lane = lax.broadcasted_iota(jnp.int32, (LANES, LANES), 1)
    group_of = {m: group for group in groups for m in group}
    for w, level in enumerate(members):
        lv = levels[level]
        group = group_of[level]
        head = sm[level * group_size + rho]
        off = rho & (lv.rate - 1)
        pick = (col_id == 2 * row_id + head % 2).astype(BF16)
        for s in range(len(sources)):
            copies[w * len(sources) + s].wait()
        tops = []
        flat = [bufs[w].at[s].reshape(2 * lv.rows, LANES) for s in range(len(sources))]
        for u in range(lv.rows // LANES):
            got = [
                plain_dot(pick, flat[s][u * 2 * LANES : (u + 1) * 2 * LANES, :])
                for s in range(len(sources))
            ]
            delta = jnp.sum(got[3] * got[4], axis=1, keepdims=True)
            start = u * LANES * lv.rate + off
            if lv.rate == 1:
                logs_u = turned[u * LANES : (u + 1) * LANES, :]
            else:
                logs_u = turned[pl.ds(start, LANES, stride=lv.rate), :]
            total = jnp.sum(jnp.where(lane == head, logs_u, 0.0), axis=1, keepdims=True) * LOG2E
            square = jnp.zeros((LANES, LANES), F32)
            for at, col in enumerate(split3(total) + split3(delta) + (total, delta)):
                square = jnp.where(lane == at, col, square)
            col_refs[w][u * LANES : (u + 1) * LANES, :] = square
            tops.append(square.T[:TAG_ROWS])
            low = [g.astype(BF16) for g in got[:4]]
            for s in range(4):
                own_refs[w][s * lv.rows + u * LANES : s * lv.rows + (u + 1) * LANES, :] = low[s]
            for bit in range(lv.bits):
                base = pack_layout(levels, group, bit)[0][level]
                later = (seq >> bit) % 2 == 1
                send = send_refs[group, bit]
                for s in range(2):
                    first = base + s * lv.rows + u * LANES
                    send[first : first + LANES, :] = jnp.where(later, low[2 + s], low[s])
        if len(tops) == 1:
            tops.append(jnp.zeros((TAG_ROWS, LANES), F32))
        tags = jnp.concatenate(tops, axis=0).astype(BF16)
        tag_refs[w][...] = tags
        for bit in range(lv.bits):
            first = pack_layout(levels, group, bit)[0][level] + 2 * lv.rows
            send_refs[group, bit][first : first + lv.tags, :] = tags


def group_bits(levels, group):
    return max(levels[m].bits for m in group)


def extract(levels, groups, group_size, sm, sources, logs):
    tokens = sources[0].shape[0]
    members = [m for group in groups for m in group]
    n = len(members)
    shapes = [jax.ShapeDtypeStruct((4 * levels[m].rows, LANES), BF16) for m in members]
    shapes += [jax.ShapeDtypeStruct((levels[m].tags, LANES), BF16) for m in members]
    shapes += [jax.ShapeDtypeStruct((levels[m].rows, LANES), F32) for m in members]
    sent = [(group, bit) for group in groups for bit in range(group_bits(levels, group))]
    shapes += [
        jax.ShapeDtypeStruct((pack_layout(levels, group, bit)[1], LANES), BF16)
        for group, bit in sent
    ]

    def kernel(*refs):
        extract_kernel(levels, groups, group_size, *refs)

    results = pl.pallas_call(
        kernel,
        out_shape=shapes,
        in_specs=[pl.BlockSpec(memory_space=pltpu.SMEM)]
        + [pl.BlockSpec(memory_space=pltpu.HBM)] * 6,
        scratch_shapes=[pltpu.VMEM((5, levels[m].rows, 2, LANES), BF16) for m in members]
        + [
            pltpu.VMEM((tokens, LANES), F32),
            pltpu.VMEM(logs.shape, F32),
            pltpu.SemaphoreType.DMA,
            pltpu.SemaphoreType.DMA((n, 5)),
        ],
        compiler_params=pltpu.CompilerParams(vmem_limit_bytes=VMEM_LIMIT),
    )(sm, *[pltpu.with_memory_space_constraint(a, pltpu.HBM) for a in (*sources, logs)])
    kept = {m: (results[w], results[n + w], results[2 * n + w]) for w, m in enumerate(members)}
    return kept, dict(zip(sent, results[3 * n :]))


def tag_row(tags, base, first_row, count, which):
    parts = []
    tile = None
    for u in range(count // LANES):
        if u % 2 == 0:
            at = pl.multiple_of(base + first_row // LANES * TAG_ROWS + u * TAG_ROWS, PAIR)
            tile = tags[pl.ds(at, PAIR), :].astype(F32)
        at = u % 2 * TAG_ROWS + which
        parts.append(tile[at : at + 1] + tile[at + 1 : at + 2] + tile[at + 2 : at + 3])
    return parts[0] if len(parts) == 1 else jnp.concatenate(parts, axis=1)


def query_side(q, g, total, delta, k, v, factor, allowed):
    scores = rows_dot(q, k)
    probs = jnp.exp2(scores * factor - total)
    if allowed is not None:
        probs = jnp.where(allowed, probs, 0.0)
    ds = (probs * (rows_dot(g, v) - delta)).astype(BF16)
    return plain_dot(ds, k)


def key_side(k, v, q, g, total, delta, factor, allowed):
    scores = rows_dot(k, q)
    probs = jnp.exp2(scores * factor - total)
    if allowed is not None:
        probs = jnp.where(allowed, probs, 0.0)
    dv = plain_dot(probs.astype(BF16), g)
    ds = (probs * (rows_dot(v, g) - delta)).astype(BF16)
    return plain_dot(ds, q), dv


class Block:
    def __init__(self, ref, first, second, tag_ref, tag_base):
        self.ref, self.first, self.second = ref, first, second
        self.tag_ref, self.tag_base = tag_ref, tag_base

    def pair(self, at, tile):
        def load(base):
            return self.ref[pl.ds(pl.multiple_of(base + at, PAIR), tile), :]

        return load(self.first), load(self.second)

    def tags(self, at, tile):
        return tuple(tag_row(self.tag_ref, self.tag_base, at, tile, which) for which in (0, 3))


def run_tiles(count, tile, step):
    if count == 1:
        step(0)
        return

    def turn(i, carry):
        step(pl.multiple_of(i * tile, tile))
        return carry

    lax.fori_loop(0, count, turn, 0)


class LevelWork:
    def __init__(self, lv, own, tags, col, acc, at, scaling):
        self.rows, self.acc, self.at, self.col = lv.rows, acc, at, col
        self.tile = min(lv.rows, 256)
        self.count = lv.rows // self.tile
        self.factor = scaling * LOG2E
        self.keys = Block(own, 0, lv.rows, None, 0)
        self.queries = Block(own, 2 * lv.rows, 3 * lv.rows, tags, 0)

    def put(self, which, at, value, add):
        first = self.at + which * self.rows + at
        where = pl.ds(pl.multiple_of(first, PAIR), self.tile)
        if add:
            self.acc[where, :] += value
        else:
            self.acc[where, :] = value

    def query_rows(self, at):
        q, g = self.queries.pair(at, self.tile)
        where = pl.ds(at, self.tile)
        return q, g, self.col[where, 6:7], self.col[where, 7:8]

    def diagonal(self):
        tile = self.tile
        tri_r = lax.broadcasted_iota(jnp.int32, (tile, tile), 0)
        tri_c = lax.broadcasted_iota(jnp.int32, (tile, tile), 1)
        for i in range(self.count):
            mine = self.query_rows(i * tile)
            sum_q = jnp.zeros((tile, LANES), F32)
            for j in range(i + 1):
                allowed = tri_c <= tri_r if i == j else None
                sum_q += query_side(*mine, *self.keys.pair(j * tile, tile), self.factor, allowed)
            self.put(0, i * tile, sum_q, False)
            mine = self.keys.pair(i * tile, tile)
            sum_k = jnp.zeros((tile, LANES), F32)
            sum_v = jnp.zeros((tile, LANES), F32)
            for j in range(i, self.count):
                allowed = tri_r <= tri_c if i == j else None
                there = self.queries.pair(j * tile, tile) + self.queries.tags(j * tile, tile)
                part = key_side(*mine, *there, self.factor, allowed)
                sum_k += part[0]
                sum_v += part[1]
            self.put(1, i * tile, sum_k, False)
            self.put(2, i * tile, sum_v, False)

    def earlier_keys(self, blocks):
        def step(at):
            mine = self.query_rows(at)
            sum_q = jnp.zeros((self.tile, LANES), F32)
            for block in blocks:
                for j in range(self.count):
                    there = block.pair(j * self.tile, self.tile)
                    sum_q += query_side(*mine, *there, self.factor, None)
            self.put(0, at, sum_q, True)

        run_tiles(self.count, self.tile, step)

    def later_queries(self, blocks):
        def step(at):
            mine = self.keys.pair(at, self.tile)
            sum_k = jnp.zeros((self.tile, LANES), F32)
            sum_v = jnp.zeros((self.tile, LANES), F32)
            for block in blocks:
                for j in range(self.count):
                    there = block.pair(j * self.tile, self.tile) + block.tags(j * self.tile, self.tile)
                    part = key_side(*mine, *there, self.factor, None)
                    sum_k += part[0]
                    sum_v += part[1]
            self.put(1, at, sum_k, True)
            self.put(2, at, sum_v, True)

        run_tiles(self.count, self.tile, step)


STAGES = {
    (0,): (("first", True, slice(0, -1), (0, 1)), ("last", False, slice(-1, None), (1, 3))),
    (1,): (("own", True, slice(0, 0), None), ("last", False, slice(0, None), (0, 3))),
    (2, 3): (
        ("own", True, slice(0, 0), None),
        ("first", False, slice(0, -1), (0, 1)),
        ("last", False, slice(-1, None), (1, 3)),
    ),
}


def compute(levels, members, group, stage, kept, received, before, scaling):
    n = len(members)
    name, own_block, chosen, parts = stage
    more = name != "last"
    bits_of = {m: list(range(levels[m].bits))[chosen] for m in members}
    bits = sorted({bit for m in members for bit in bits_of[m]})
    steps = [k for k in sorted(received) if k.bit_length() - 1 in bits]
    rows_sum = sum(levels[m].rows for m in members)
    given = [kept[m][part] for part in range(3) for m in members]
    given += [received[k] for k in steps]
    if before is not None:
        given.append(before)
    inputs = len(given)
    low, high = parts or (0, 0)
    shapes = []
    if parts:
        shapes.append(jax.ShapeDtypeStruct(((high - low) * rows_sum, LANES), BF16))
    if more:
        shapes.append(jax.ShapeDtypeStruct((3 * rows_sum, LANES), F32))

    def kernel(*refs):
        own_refs, tag_refs, col_refs = refs[:n], refs[n : 2 * n], refs[2 * n : 3 * n]
        got = dict(zip(steps, refs[3 * n :]))
        out, acc = refs[inputs], refs[inputs + (1 if parts else 0)]
        seq = lax.axis_index("seq")
        if before is not None:
            acc[...] = refs[inputs - 1][...]
        work, at = [], 0
        for w, level in enumerate(members):
            lv = levels[level]
            work.append(LevelWork(lv, own_refs[w], tag_refs[w], col_refs[w], acc, at, scaling))
            at += 3 * lv.rows
        if own_block:
            for each in work:
                each.diagonal()
        for bit in bits:
            later = (seq >> bit) % 2 == 1
            offsets = pack_layout(levels, group, bit)[0]
            todo = []
            for w, level in enumerate(members):
                if bit in bits_of[level]:
                    rows, base = levels[level].rows, offsets[level]
                    todo.append(
                        (
                            work[w],
                            [
                                Block(got[k], base, base + rows, got[k], base + 2 * rows)
                                for k in range(2**bit, 2 ** (bit + 1))
                            ],
                        )
                    )

            @pl.when(later)
            def _(todo=todo):
                for each, blocks in todo:
                    each.earlier_keys(blocks)

            @pl.when(jnp.logical_not(later))
            def _(todo=todo):
                for each, blocks in todo:
                    each.later_queries(blocks)

        at, put = 0, 0
        for level in members:
            lv = levels[level]
            top = (seq >> (lv.bits - 1)) % 2 == 1
            for place_at in range(low, high):
                when_low, when_high = place_at, (place_at + 2) % 3
                value = jnp.where(
                    top,
                    acc[at + when_high * lv.rows : at + (when_high + 1) * lv.rows, :],
                    acc[at + when_low * lv.rows : at + (when_low + 1) * lv.rows, :],
                )
                factor = jnp.where(
                    top, 1.0 if when_high == 2 else scaling, 1.0 if when_low == 2 else scaling
                )
                out[put : put + lv.rows, :] = (value * factor).astype(BF16)
                put += lv.rows
            at += 3 * lv.rows

    return pl.pallas_call(
        kernel,
        out_shape=shapes,
        in_specs=[pl.BlockSpec(memory_space=pltpu.VMEM)] * inputs,
        scratch_shapes=[] if more else [pltpu.VMEM((3 * rows_sum, LANES), F32)],
        compiler_params=pltpu.CompilerParams(vmem_limit_bytes=VMEM_LIMIT),
    )(*given)


def place(levels, group_size, heads_here, local_tokens, sm, gathered):
    rates = len(gathered[0][0][2])
    flat = [array for pieces in gathered for piece in pieces for array in piece[2]]
    block, half = 2 * LANES, LANES // 2
    parts = block // half
    steps = local_tokens // block
    tall = heads_here * half

    def kernel(sm_ref, *refs):
        sources = refs[: len(flat)]
        outs = refs[len(flat) : len(flat) + 3]
        spread, buf, table, sems = refs[len(flat) + 3 :]
        step = pl.program_id(0)
        rho = lax.axis_index("rate")

        @pl.when(step == 0)
        def _():
            slots = []
            for i in range(heads_here):
                slot = jnp.int32(0)
                for s in range(HEADS):
                    slot = jnp.where(sm_ref[s] == rho * heads_here + i, s, slot)
                slots.append(slot)
                table[i] = slot // group_size
            shifts = [slot // group_size for slot in slots]
            for i in range(heads_here):
                for level in range(1, LEVELS):
                    end = 3 * levels[level].rows
                    buf[i, end : end + half, :] = jnp.zeros((half, LANES), BF16)

            for i in range(heads_here):
                lane_i = slots[i] % group_size
                first = 0
                for g, members in enumerate(GROUPS):
                    above = 0
                    for level in members:
                        rows = levels[level].rows
                        for x in range(rates):
                            hit = jnp.logical_and(shifts[i] == level, lane_i == rho ^ x)

                            @pl.when(hit)
                            def _(i=i, pieces=gathered[g], first=first, x=x, above=above, rows=rows):
                                for p, (low, high, _) in enumerate(pieces):
                                    source = sources[first + p * rates + x]
                                    size = (high - low) * rows
                                    pltpu.make_async_copy(
                                        source.at[pl.ds(above * (high - low), size)],
                                        buf.at[i, pl.ds(low * rows, size)],
                                        sems.at[i],
                                    ).start()

                        above += rows
                    first += rates * len(gathered[g])

            row_id = lax.broadcasted_iota(jnp.int32, (tall, half), 0)
            col_id = lax.broadcasted_iota(jnp.int32, (tall, half), 1)
            for part in range(2):
                for i in range(heads_here):
                    rate = 1 << shifts[i]
                    off = (slots[i] % group_size) & (rate - 1)
                    first = jnp.where(shifts[i] == 0, 0, part * half)
                    token = col_id * rate + (off - first)
                    hit = row_id == token * heads_here + i
                    spread[part, :, i * half : (i + 1) * half] = hit.astype(BF16)
            for i in range(heads_here):
                for level in range(LEVELS):
                    rows = 3 * levels[level].rows

                    @pl.when(shifts[i] == level)
                    def _(i=i, rows=rows):
                        there = buf.at[i, pl.ds(0, rows)]
                        pltpu.make_async_copy(there, there, sems.at[i]).wait()

        shifts = [table[i] for i in range(heads_here)]
        seq = lax.axis_index("seq")
        tops = []
        for i in range(heads_here):
            top = jnp.int32(0)
            for level in range(LEVELS):
                bit = (seq >> (levels[level].bits - 1)) & 1
                top = jnp.where(shifts[i] == level, bit, top)
            tops.append(top)

        for part in range(parts):
            columns = []
            for which in range(3):
                rows = []
                for i in range(heads_here):
                    turned = jnp.where(tops[i] == 1, (which + 1) % 3, which)
                    at = turned * (local_tokens >> shifts[i]) + step * (block >> shifts[i])
                    at += part // 2 * (2 * half >> shifts[i])
                    at += jnp.where(shifts[i] == 0, part % 2 * half, 0)
                    rows.append(buf[i, pl.ds(pl.multiple_of(at, PAIR), half), :])
                columns.append(jnp.concatenate(rows, axis=0))
            two = plain_dot(spread[part % 2], jnp.concatenate(columns[:2], axis=1))
            where = pl.ds(part * tall, tall)
            outs[0][where, :] = two[:, :LANES].astype(BF16)
            outs[1][where, :] = two[:, LANES:].astype(BF16)
            outs[2][where, :] = plain_dot(spread[part % 2], columns[2]).astype(BF16)

    shape = jax.ShapeDtypeStruct((local_tokens * heads_here, LANES), BF16)
    spec = pl.BlockSpec((block * heads_here, LANES), lambda i: (i, 0))
    results = pl.pallas_call(
        kernel,
        grid=(steps,),
        out_shape=[shape] * 3,
        in_specs=[pl.BlockSpec(memory_space=pltpu.SMEM)]
        + [pl.BlockSpec(memory_space=pl.ANY)] * len(flat),
        out_specs=[spec] * 3,
        scratch_shapes=[
            pltpu.VMEM((2, tall, tall), BF16),
            pltpu.VMEM((heads_here, 3 * local_tokens + block, LANES), BF16),
            pltpu.SMEM((heads_here,), jnp.int32),
            pltpu.SemaphoreType.DMA((heads_here,)),
        ],
        compiler_params=pltpu.CompilerParams(vmem_limit_bytes=VMEM_LIMIT),
        name="place",
    )(sm, *flat)
    return tuple(r.reshape(local_tokens, heads_here, LANES) for r in results)


def body(queries, key_rows, values, attn_out, out_grad, log_totals, assignment):
    local_tokens = queries.shape[0]
    scaling = queries.shape[2] ** (-0.5)
    rate_count = lax.axis_size("rate")
    seq_count = lax.axis_size("seq")
    group_size = HEADS // LEVELS
    levels = [Level(c, local_tokens, local_tokens * seq_count) for c in range(LEVELS)]
    paired = [
        a.reshape(local_tokens, HEADS // 2, 2, LANES)
        for a in (key_rows, values, queries, out_grad, attn_out)
    ]
    logs = log_totals.T
    received = {}
    kept = {}
    for group in SENDS:
        some, sends = extract(levels, (group,), group_size, assignment, paired, logs)
        kept.update(some)
        received[group] = {}
        for k in range(1, 2 ** group_bits(levels, group)):
            received[group][k] = swapped(sends[group, k.bit_length() - 1], "seq", k)
    gathered = []
    for members in GROUPS:
        group = next(g for g in SENDS if members[0] in g)
        pieces, before = [], None
        for stage in STAGES[members]:
            results = compute(levels, members, group, stage, kept, received[group], before, scaling)
            before = results[-1]
            if stage[3]:
                mine = results[0]
                far = swapped(mine, "rate", 2)
                near = swapped(mine, "rate", 1)
                pieces.append((*stage[3], [mine, near, far, swapped(far, "rate", 1)]))
        gathered.append(pieces)
    return place(levels, group_size, HEADS // rate_count, local_tokens, assignment, gathered)


def solution(mesh):
    placed = (P("seq", None, None),) * 5 + (P("seq", None), P())
    return jax.shard_map(
        body,
        mesh=mesh,
        in_specs=placed,
        out_specs=(P("seq", "rate", None),) * 3,
        check_vma=False,
    )
```

```python
import math

import jax
import jax.numpy as jnp
from jax import lax
from jax.experimental import pallas as pl
from jax.experimental.pallas import tpu as pltpu
from jax.sharding import PartitionSpec as P


HEADS = 16
SEG = 2048
LEVELS = 4
GROUPS = ((0,), (1,), (2, 3))
SENDS = ((0,), (1, 2, 3))
VMEM_LIMIT = 24 * 1024 * 1024
LANES = 128
TAG_ROWS = 8
PAIR = 16
COPY_ROWS = 1024
LOG2E = math.log2(math.e)


F32 = jnp.float32
BF16 = jnp.bfloat16


def swapped(array, axis, by):
    devices = lax.axis_size(axis)
    return lax.ppermute(array, axis, [(i, i ^ by) for i in range(devices)])


def rows_dot(a, b):
    return lax.dot_general(a, b, (((1,), (1,)), ((), ())), preferred_element_type=F32)


def plain_dot(a, b):
    return jnp.dot(a, b, preferred_element_type=F32)


class Level:
    def __init__(self, level, local_tokens, all_tokens):
        self.rate = 2**level
        self.rows = local_tokens // self.rate
        self.span = min(SEG, all_tokens // self.rate) * self.rate // local_tokens
        self.bits = self.span.bit_length() - 1
        self.tags = max(self.rows // LANES * TAG_ROWS, PAIR)
        self.pack_rows = 2 * self.rows + self.tags


def pack_layout(levels, members, bit):
    at, offsets = 0, {}
    for level in members:
        if bit < levels[level].bits:
            offsets[level] = at
            at += levels[level].pack_rows
    return offsets, at


def split3(col):
    hi = col.astype(BF16).astype(F32)
    rest = col - hi
    mid = rest.astype(BF16).astype(F32)
    return hi, mid, rest - mid


def copy_rows(lv):
    return min(lv.rows, COPY_ROWS)


def extract_kernel(levels, groups, group_size, sm, keys, values, queries, grads, outs, logs, *refs):
    members = [m for group in groups for m in group]
    n = len(members)
    own_refs, tag_refs, col_refs = refs[:n], refs[n : 2 * n], refs[2 * n : 3 * n]
    at = 3 * n
    send_refs = {}
    for group in groups:
        for bit in range(group_bits(levels, group)):
            send_refs[group, bit] = refs[at]
            at += 1
    bufs = refs[at : at + n]
    turned, logs_buf, logs_sem, sems = refs[at + n :]
    rho, seq = lax.axis_index("rate"), lax.axis_index("seq")
    tokens = keys.shape[0]
    sources = (keys, values, queries, grads, outs)
    copies = []
    for w, level in enumerate(members):
        rate, rows = levels[level].rate, levels[level].rows
        head = sm[level * group_size + rho]
        off = rho & (rate - 1)
        piece = copy_rows(levels[level])
        for u in range(0, rows, piece):
            for s, source in enumerate(sources):
                picked = source.reshape(rows, rate, HEADS // 2, 2, LANES)
                copy = pltpu.make_async_copy(
                    picked.at[pl.ds(u, piece), off, head // 2],
                    bufs[w].at[s, pl.ds(u, piece)],
                    sems.at[len(copies)],
                )
                copy.start()
                copies.append(copy)
        if w == 0:
            logs_copy = pltpu.make_async_copy(logs, logs_buf, logs_sem)
            logs_copy.start()
    logs_copy.wait()
    for u in range(tokens // LANES):
        part = logs_buf[:, u * LANES : (u + 1) * LANES]
        square = jnp.concatenate([part, jnp.zeros((LANES - HEADS, LANES), F32)], axis=0)
        turned[u * LANES : (u + 1) * LANES, :] = square.T
    row_id = lax.broadcasted_iota(jnp.int32, (LANES, 2 * LANES), 0)
    col_id = lax.broadcasted_iota(jnp.int32, (LANES, 2 * LANES), 1)
    lane = lax.broadcasted_iota(jnp.int32, (LANES, LANES), 1)
    group_of = {m: group for group in groups for m in group}
    waited = 0
    for w, level in enumerate(members):
        lv = levels[level]
        group = group_of[level]
        head = sm[level * group_size + rho]
        off = rho & (lv.rate - 1)
        pick = (col_id == 2 * row_id + head % 2).astype(BF16)
        tops = []
        flat = [bufs[w].at[s].reshape(2 * lv.rows, LANES) for s in range(len(sources))]
        for u in range(lv.rows // LANES):
            if u * LANES % copy_rows(lv) == 0:
                for copy in copies[waited : waited + len(sources)]:
                    copy.wait()
                waited += len(sources)
            got = [
                plain_dot(pick, flat[s][u * 2 * LANES : (u + 1) * 2 * LANES, :])
                for s in range(len(sources))
            ]
            delta = jnp.sum(got[3] * got[4], axis=1, keepdims=True)
            start = u * LANES * lv.rate + off
            if lv.rate == 1:
                logs_u = turned[u * LANES : (u + 1) * LANES, :]
            else:
                logs_u = turned[pl.ds(start, LANES, stride=lv.rate), :]
            total = jnp.sum(jnp.where(lane == head, logs_u, 0.0), axis=1, keepdims=True) * LOG2E
            square = jnp.zeros((LANES, LANES), F32)
            for at, col in enumerate(split3(total) + split3(delta) + (total, delta)):
                square = jnp.where(lane == at, col, square)
            col_refs[w][u * LANES : (u + 1) * LANES, :] = square
            tops.append(square.T[:TAG_ROWS])
            low = [g.astype(BF16) for g in got[:4]]
            for s in range(4):
                own_refs[w][s * lv.rows + u * LANES : s * lv.rows + (u + 1) * LANES, :] = low[s]
            for bit in range(lv.bits):
                base = pack_layout(levels, group, bit)[0][level]
                later = (seq >> bit) % 2 == 1
                send = send_refs[group, bit]
                for s in range(2):
                    first = base + s * lv.rows + u * LANES
                    send[first : first + LANES, :] = jnp.where(later, low[2 + s], low[s])
        if len(tops) == 1:
            tops.append(jnp.zeros((TAG_ROWS, LANES), F32))
        tags = jnp.concatenate(tops, axis=0).astype(BF16)
        tag_refs[w][...] = tags
        for bit in range(lv.bits):
            first = pack_layout(levels, group, bit)[0][level] + 2 * lv.rows
            send_refs[group, bit][first : first + lv.tags, :] = tags


def group_bits(levels, group):
    return max(levels[m].bits for m in group)


def extract(levels, groups, group_size, sm, sources, logs):
    tokens = sources[0].shape[0]
    members = [m for group in groups for m in group]
    n = len(members)
    shapes = [jax.ShapeDtypeStruct((4 * levels[m].rows, LANES), BF16) for m in members]
    shapes += [jax.ShapeDtypeStruct((levels[m].tags, LANES), BF16) for m in members]
    shapes += [jax.ShapeDtypeStruct((levels[m].rows, LANES), F32) for m in members]
    sent = [(group, bit) for group in groups for bit in range(group_bits(levels, group))]
    shapes += [
        jax.ShapeDtypeStruct((pack_layout(levels, group, bit)[1], LANES), BF16)
        for group, bit in sent
    ]

    def kernel(*refs):
        extract_kernel(levels, groups, group_size, *refs)

    results = pl.pallas_call(
        kernel,
        out_shape=shapes,
        in_specs=[pl.BlockSpec(memory_space=pltpu.SMEM)]
        + [pl.BlockSpec(memory_space=pltpu.HBM)] * 6,
        scratch_shapes=[pltpu.VMEM((5, levels[m].rows, 2, LANES), BF16) for m in members]
        + [
            pltpu.VMEM((tokens, LANES), F32),
            pltpu.VMEM(logs.shape, F32),
            pltpu.SemaphoreType.DMA,
            pltpu.SemaphoreType.DMA(
                (5 * sum(levels[m].rows // copy_rows(levels[m]) for m in members),)
            ),
        ],
        compiler_params=pltpu.CompilerParams(vmem_limit_bytes=VMEM_LIMIT),
    )(sm, *[pltpu.with_memory_space_constraint(a, pltpu.HBM) for a in (*sources, logs)])
    kept = {m: (results[w], results[n + w], results[2 * n + w]) for w, m in enumerate(members)}
    return kept, dict(zip(sent, results[3 * n :]))


def tag_row(tags, base, first_row, count, which):
    parts = []
    tile = None
    for u in range(count // LANES):
        if u % 2 == 0:
            at = pl.multiple_of(base + first_row // LANES * TAG_ROWS + u * TAG_ROWS, PAIR)
            tile = tags[pl.ds(at, PAIR), :].astype(F32)
        at = u % 2 * TAG_ROWS + which
        parts.append(tile[at : at + 1] + tile[at + 1 : at + 2] + tile[at + 2 : at + 3])
    return parts[0] if len(parts) == 1 else jnp.concatenate(parts, axis=1)


def query_side(q, g, total, delta, k, v, factor, allowed):
    scores = rows_dot(q, k)
    probs = jnp.exp2(scores * factor - total)
    if allowed is not None:
        probs = jnp.where(allowed, probs, 0.0)
    ds = (probs * (rows_dot(g, v) - delta)).astype(BF16)
    return plain_dot(ds, k)


def key_side(k, v, q, g, total, delta, factor, allowed):
    scores = rows_dot(k, q)
    probs = jnp.exp2(scores * factor - total)
    if allowed is not None:
        probs = jnp.where(allowed, probs, 0.0)
    dv = plain_dot(probs.astype(BF16), g)
    ds = (probs * (rows_dot(v, g) - delta)).astype(BF16)
    return plain_dot(ds, q), dv


class Block:
    def __init__(self, ref, first, second, tag_ref, tag_base):
        self.ref, self.first, self.second = ref, first, second
        self.tag_ref, self.tag_base = tag_ref, tag_base

    def pair(self, at, tile):
        def load(base):
            return self.ref[pl.ds(pl.multiple_of(base + at, PAIR), tile), :]

        return load(self.first), load(self.second)

    def tags(self, at, tile):
        return tuple(tag_row(self.tag_ref, self.tag_base, at, tile, which) for which in (0, 3))


def run_tiles(count, tile, step):
    if count == 1:
        step(0)
        return

    def turn(i, carry):
        step(pl.multiple_of(i * tile, tile))
        return carry

    lax.fori_loop(0, count, turn, 0)


class LevelWork:
    def __init__(self, lv, own, tags, col, acc, at, scaling):
        self.rows, self.acc, self.at, self.col = lv.rows, acc, at, col
        self.tile = min(lv.rows, 256)
        self.count = lv.rows // self.tile
        self.factor = scaling * LOG2E
        self.keys = Block(own, 0, lv.rows, None, 0)
        self.queries = Block(own, 2 * lv.rows, 3 * lv.rows, tags, 0)

    def put(self, which, at, value, add):
        first = self.at + which * self.rows + at
        where = pl.ds(pl.multiple_of(first, PAIR), self.tile)
        if add:
            self.acc[where, :] += value
        else:
            self.acc[where, :] = value

    def query_rows(self, at):
        q, g = self.queries.pair(at, self.tile)
        where = pl.ds(at, self.tile)
        return q, g, self.col[where, 6:7], self.col[where, 7:8]

    def diagonal(self):
        tile = self.tile
        tri_r = lax.broadcasted_iota(jnp.int32, (tile, tile), 0)
        tri_c = lax.broadcasted_iota(jnp.int32, (tile, tile), 1)
        for i in range(self.count):
            mine = self.query_rows(i * tile)
            sum_q = jnp.zeros((tile, LANES), F32)
            for j in range(i + 1):
                allowed = tri_c <= tri_r if i == j else None
                sum_q += query_side(*mine, *self.keys.pair(j * tile, tile), self.factor, allowed)
            self.put(0, i * tile, sum_q, False)
            mine = self.keys.pair(i * tile, tile)
            sum_k = jnp.zeros((tile, LANES), F32)
            sum_v = jnp.zeros((tile, LANES), F32)
            for j in range(i, self.count):
                allowed = tri_r <= tri_c if i == j else None
                there = self.queries.pair(j * tile, tile) + self.queries.tags(j * tile, tile)
                part = key_side(*mine, *there, self.factor, allowed)
                sum_k += part[0]
                sum_v += part[1]
            self.put(1, i * tile, sum_k, False)
            self.put(2, i * tile, sum_v, False)

    def earlier_keys(self, blocks):
        def step(at):
            mine = self.query_rows(at)
            sum_q = jnp.zeros((self.tile, LANES), F32)
            for block in blocks:
                for j in range(self.count):
                    there = block.pair(j * self.tile, self.tile)
                    sum_q += query_side(*mine, *there, self.factor, None)
            self.put(0, at, sum_q, True)

        run_tiles(self.count, self.tile, step)

    def later_queries(self, blocks):
        def step(at):
            mine = self.keys.pair(at, self.tile)
            sum_k = jnp.zeros((self.tile, LANES), F32)
            sum_v = jnp.zeros((self.tile, LANES), F32)
            for block in blocks:
                for j in range(self.count):
                    there = block.pair(j * self.tile, self.tile) + block.tags(j * self.tile, self.tile)
                    part = key_side(*mine, *there, self.factor, None)
                    sum_k += part[0]
                    sum_v += part[1]
            self.put(1, at, sum_k, True)
            self.put(2, at, sum_v, True)

        run_tiles(self.count, self.tile, step)


STAGES = {
    (0,): (("first", True, slice(0, -1), (0, 1), (0, 1)), ("last", False, slice(-1, None), (0, 1), (1, 3))),
    (1,): (("own", True, slice(0, 0), (), None), ("last", False, slice(0, None), (0, 1), (0, 3))),
    (2, 3): (
        ("own", True, slice(0, 0), (), None),
        ("first", False, slice(0, -1), (0, 1), (0, 1)),
        ("next", False, slice(-1, None), (0,), None),
        ("last", False, slice(-1, None), (1,), (1, 3)),
    ),
}


def compute(levels, members, group, stage, kept, received, before, scaling):
    n = len(members)
    name, own_block, chosen, odd, parts = stage
    more = name != "last"
    bits_of = {m: list(range(levels[m].bits))[chosen] for m in members}
    bits = sorted({bit for m in members for bit in bits_of[m]})
    steps = [k for k in sorted(received) if k.bit_length() - 1 in bits and k % 2 in odd]
    rows_sum = sum(levels[m].rows for m in members)
    given = [kept[m][part] for part in range(3) for m in members]
    given += [received[k] for k in steps]
    if before is not None:
        given.append(before)
    inputs = len(given)
    low, high = parts or (0, 0)
    shapes = []
    if parts:
        shapes.append(jax.ShapeDtypeStruct(((high - low) * rows_sum, LANES), BF16))
    if more:
        shapes.append(jax.ShapeDtypeStruct((3 * rows_sum, LANES), F32))

    def kernel(*refs):
        own_refs, tag_refs, col_refs = refs[:n], refs[n : 2 * n], refs[2 * n : 3 * n]
        got = dict(zip(steps, refs[3 * n :]))
        out, acc = refs[inputs], refs[inputs + (1 if parts else 0)]
        seq = lax.axis_index("seq")
        if before is not None:
            acc[...] = refs[inputs - 1][...]
        work, at = [], 0
        for w, level in enumerate(members):
            lv = levels[level]
            work.append(LevelWork(lv, own_refs[w], tag_refs[w], col_refs[w], acc, at, scaling))
            at += 3 * lv.rows
        if own_block:
            for each in work:
                each.diagonal()
        for bit in bits:
            later = (seq >> bit) % 2 == 1
            offsets = pack_layout(levels, group, bit)[0]
            todo = []
            for w, level in enumerate(members):
                if bit in bits_of[level]:
                    rows, base = levels[level].rows, offsets[level]
                    todo.append(
                        (
                            work[w],
                            [
                                Block(got[k], base, base + rows, got[k], base + 2 * rows)
                                for k in range(2**bit, 2 ** (bit + 1))
                                if k in got
                            ],
                        )
                    )

            @pl.when(later)
            def _(todo=todo):
                for each, blocks in todo:
                    each.earlier_keys(blocks)

            @pl.when(jnp.logical_not(later))
            def _(todo=todo):
                for each, blocks in todo:
                    each.later_queries(blocks)

        at, put = 0, 0
        for level in members:
            lv = levels[level]
            top = (seq >> (lv.bits - 1)) % 2 == 1
            for place_at in range(low, high):
                when_low, when_high = place_at, (place_at + 2) % 3
                value = jnp.where(
                    top,
                    acc[at + when_high * lv.rows : at + (when_high + 1) * lv.rows, :],
                    acc[at + when_low * lv.rows : at + (when_low + 1) * lv.rows, :],
                )
                factor = jnp.where(
                    top, 1.0 if when_high == 2 else scaling, 1.0 if when_low == 2 else scaling
                )
                out[put : put + lv.rows, :] = (value * factor).astype(BF16)
                put += lv.rows
            at += 3 * lv.rows

    return pl.pallas_call(
        kernel,
        out_shape=shapes,
        in_specs=[pl.BlockSpec(memory_space=pltpu.VMEM)] * inputs,
        scratch_shapes=[] if more else [pltpu.VMEM((3 * rows_sum, LANES), F32)],
        compiler_params=pltpu.CompilerParams(vmem_limit_bytes=VMEM_LIMIT),
    )(*given)


def place(levels, group_size, heads_here, local_tokens, sm, gathered):
    rates = len(gathered[0][0][2])
    flat = [array for pieces in gathered for piece in pieces for array in piece[2]]
    block, half = 4 * LANES, LANES // 2
    parts = block // half
    steps = local_tokens // block
    tall = heads_here * half

    def kernel(sm_ref, *refs):
        sources = refs[: len(flat)]
        outs = refs[len(flat) : len(flat) + 3]
        spread, buf, table, sems = refs[len(flat) + 3 :]
        step = pl.program_id(0)
        rho = lax.axis_index("rate")

        @pl.when(step == 0)
        def _():
            slots = []
            for i in range(heads_here):
                slot = jnp.int32(0)
                for s in range(HEADS):
                    slot = jnp.where(sm_ref[s] == rho * heads_here + i, s, slot)
                slots.append(slot)
                table[i] = slot // group_size
            shifts = [slot // group_size for slot in slots]
            for i in range(heads_here):
                for level in range(1, LEVELS):
                    end = 3 * levels[level].rows
                    buf[i, end : end + half, :] = jnp.zeros((half, LANES), BF16)

            for i in range(heads_here):
                lane_i = slots[i] % group_size
                first = 0
                for g, members in enumerate(GROUPS):
                    above = 0
                    for level in members:
                        rows = levels[level].rows
                        for x in range(rates):
                            hit = jnp.logical_and(shifts[i] == level, lane_i == rho ^ x)

                            @pl.when(hit)
                            def _(i=i, pieces=gathered[g], first=first, x=x, above=above, rows=rows):
                                for p, (low, high, _) in enumerate(pieces):
                                    source = sources[first + p * rates + x]
                                    size = (high - low) * rows
                                    pltpu.make_async_copy(
                                        source.at[pl.ds(above * (high - low), size)],
                                        buf.at[i, pl.ds(low * rows, size)],
                                        sems.at[i],
                                    ).start()

                        above += rows
                    first += rates * len(gathered[g])

            row_id = lax.broadcasted_iota(jnp.int32, (tall, half), 0)
            col_id = lax.broadcasted_iota(jnp.int32, (tall, half), 1)
            for part in range(2):
                for i in range(heads_here):
                    rate = 1 << shifts[i]
                    off = (slots[i] % group_size) & (rate - 1)
                    first = jnp.where(shifts[i] == 0, 0, part * half)
                    token = col_id * rate + (off - first)
                    hit = row_id == token * heads_here + i
                    spread[part, :, i * half : (i + 1) * half] = hit.astype(BF16)
            for i in range(heads_here):
                for level in range(LEVELS):
                    rows = 3 * levels[level].rows

                    @pl.when(shifts[i] == level)
                    def _(i=i, rows=rows):
                        there = buf.at[i, pl.ds(0, rows)]
                        pltpu.make_async_copy(there, there, sems.at[i]).wait()

        shifts = [table[i] for i in range(heads_here)]
        seq = lax.axis_index("seq")
        tops = []
        for i in range(heads_here):
            top = jnp.int32(0)
            for level in range(LEVELS):
                bit = (seq >> (levels[level].bits - 1)) & 1
                top = jnp.where(shifts[i] == level, bit, top)
            tops.append(top)

        for part in range(parts):
            columns = []
            for which in range(3):
                rows = []
                for i in range(heads_here):
                    turned = jnp.where(tops[i] == 1, (which + 1) % 3, which)
                    at = turned * (local_tokens >> shifts[i]) + step * (block >> shifts[i])
                    at += part // 2 * (2 * half >> shifts[i])
                    at += jnp.where(shifts[i] == 0, part % 2 * half, 0)
                    rows.append(buf[i, pl.ds(pl.multiple_of(at, PAIR), half), :])
                columns.append(jnp.concatenate(rows, axis=0))
            two = plain_dot(spread[part % 2], jnp.concatenate(columns[:2], axis=1))
            where = pl.ds(part * tall, tall)
            outs[0][where, :] = two[:, :LANES].astype(BF16)
            outs[1][where, :] = two[:, LANES:].astype(BF16)
            outs[2][where, :] = plain_dot(spread[part % 2], columns[2]).astype(BF16)

    shape = jax.ShapeDtypeStruct((local_tokens * heads_here, LANES), BF16)
    spec = pl.BlockSpec((block * heads_here, LANES), lambda i: (i, 0))
    results = pl.pallas_call(
        kernel,
        grid=(steps,),
        out_shape=[shape] * 3,
        in_specs=[pl.BlockSpec(memory_space=pltpu.SMEM)]
        + [pl.BlockSpec(memory_space=pl.ANY)] * len(flat),
        out_specs=[spec] * 3,
        scratch_shapes=[
            pltpu.VMEM((2, tall, tall), BF16),
            pltpu.VMEM((heads_here, 3 * local_tokens + block, LANES), BF16),
            pltpu.SMEM((heads_here,), jnp.int32),
            pltpu.SemaphoreType.DMA((heads_here,)),
        ],
        compiler_params=pltpu.CompilerParams(vmem_limit_bytes=VMEM_LIMIT),
        name="place",
    )(sm, *flat)
    return tuple(r.reshape(local_tokens, heads_here, LANES) for r in results)


def body(queries, key_rows, values, attn_out, out_grad, log_totals, assignment):
    local_tokens = queries.shape[0]
    scaling = queries.shape[2] ** (-0.5)
    rate_count = lax.axis_size("rate")
    seq_count = lax.axis_size("seq")
    group_size = HEADS // LEVELS
    levels = [Level(c, local_tokens, local_tokens * seq_count) for c in range(LEVELS)]
    paired = [
        a.reshape(local_tokens, HEADS // 2, 2, LANES)
        for a in (key_rows, values, queries, out_grad, attn_out)
    ]
    logs = log_totals.T
    received = {}
    kept = {}
    for group in SENDS:
        some, sends = extract(levels, (group,), group_size, assignment, paired, logs)
        kept.update(some)
        received[group] = {}
        for k in range(1, 2 ** group_bits(levels, group)):
            received[group][k] = swapped(sends[group, k.bit_length() - 1], "seq", k)
    gathered = []
    for members in GROUPS:
        group = next(g for g in SENDS if members[0] in g)
        pieces, before = [], None
        for stage in STAGES[members]:
            results = compute(levels, members, group, stage, kept, received[group], before, scaling)
            before = results[-1]
            if stage[4]:
                mine = results[0]
                far = swapped(mine, "rate", 2)
                near = swapped(mine, "rate", 1)
                pieces.append((*stage[4], [mine, near, far, swapped(far, "rate", 1)]))
        gathered.append(pieces)
    return place(levels, group_size, HEADS // rate_count, local_tokens, assignment, gathered)


def solution(mesh):
    placed = (P("seq", None, None),) * 5 + (P("seq", None), P())
    return jax.shard_map(
        body,
        mesh=mesh,
        in_specs=placed,
        out_specs=(P("seq", "rate", None),) * 3,
        check_vma=False,
    )
```
